32 devices in a mesh: grp: 2 (over y), gz: 4 (over z), gx: 2 (over x), row: 2 (over core).
Axes of the slice: x: 2, y: 2, z: 4, core: 2. Of those that a mesh axis runs over, the one named last changes fastest.
Arguments:
- volume: float32 [32, 512, 512], P(('grp', 'gz'), 'gx', 'row'), parts along dimension 0, may hold values from -6 to 6
- tile_table: bfloat16 [64, 128, 128], replicated, may hold values from -0.09375 to 0.09375
- tile_ids: int32 [4, 2, 2, 4, 32], P('gz', 'gx', 'row'), may hold values from 0 to 63
- block_ids: int32 [4, 2, 2, 4, 768], P('gz', 'gx', 'row'), may hold values from 0 to 2047
- live_slots: int32 [4, 2, 2, 4], P('gz', 'gx', 'row'), may hold values from 4 to 32, as said below
- measured: float32 [8, 512, 16], P(('grp', 'gz'), ('gx', 'row')), parts along dimension 0, may hold values from -12 to 12
- row_norm: float32 [4, 512, 16], P('gz', ('gx', 'row')), may hold values from 0.2 to 1
- col_norm: float32 [16, 512, 512], P('gz', 'gx', 'row'), may hold values from 0.5 to 2
Outputs:
- new_volume: float32 [32, 512, 512], P(('grp', 'gz'), 'gx', 'row'), parts along dimension 0
The draws below stay inside these ranges and needn't reach their ends.
There are 2 independent parts, one for each index of `grp`. The reference program is written for one: setup_inputs(seed, part) draws one part's arguments, and reference() takes and returns one part's arrays. A program takes and returns all parts, laid end to end along the dimension named above; an argument that names none is the same for every part. Nothing has to cross between parts.
Inputs may be any that keep to these rules, and one draw needn't show every extreme that they name: `block_ids`: indices of voxel blocks of the piece itself. `live_slots`: 32 is reached by some angle of some piece in every draw.
All inputs are finite; a program needn't handle non-finite values.
Results may differ from the reference program's by a relative error of at most 0.004.
Values may be sent and summed in bfloat16 or wider, within the bound.
A program may use at most 64 MiB of HBM per device.

```python
import math
import jax
import jax.numpy as jnp
from jax import lax

SIDE = 512
DET_U = 512
TILE = 128
SLAB_Z = 4
SLOTS = 32
NTILES = 64
SLABS = 4
COLS = 2
HALVES = 2
ANGLES = 4
NZ = 16
WIN = 6
UBLK = 4
XCOL = 256
YHALF = 256
NBLK = 2048


def draw_live_slots(key, part):
    key_caps, key_top, key_fill, key_angle = jax.random.split(key, 4)
    piece_count = SLABS * COLS * HALVES
    least_cap = max(1, SLOTS // 4)
    piece_caps = jax.random.randint(key_caps, (piece_count,), least_cap, SLOTS + 1)
    top_piece = jax.random.randint(key_top, (), 0, piece_count)
    piece_caps = jnp.where(jnp.arange(piece_count) == top_piece, SLOTS, piece_caps)
    lower_bound = (piece_caps + 1) // 2
    random_bits = jax.random.randint(key_fill, (piece_count, ANGLES), 0, 1 << 20)
    counts = lower_bound[:, None] + random_bits % (piece_caps - lower_bound + 1)[:, None]
    top_angle = jax.random.randint(key_angle, (piece_count,), 0, ANGLES)
    counts = jnp.where(jnp.arange(ANGLES)[None, :] == top_angle[:, None], piece_caps[:, None], counts)
    return counts.reshape(SLABS, COLS, HALVES, ANGLES).astype(jnp.int32)


def place_ends(values, key, least, high):
    spot = [jax.random.randint(jax.random.fold_in(key, axis), (), 0, length) for axis, length in enumerate(values.shape)]
    widest = values.shape.index(max(values.shape))
    beside = spot[:widest] + [(spot[widest] + 1) % values.shape[widest]] + spot[widest + 1:]
    return values.at[tuple(spot)].set(least).at[tuple(beside)].set(high)


def shard_levels(own_key, extent, cuts, least, largest):
    def one(axis_at, parts):
        heights = jax.random.uniform(jax.random.fold_in(jax.random.fold_in(own_key, 6), axis_at), (parts,), jnp.float32, least / len(cuts), largest / len(cuts))
        return jnp.repeat(jnp.exp(heights), extent[axis_at] // parts).reshape((-1,) + (1,) * (len(extent) - axis_at - 1))

    loudness = one(*cuts[0])
    for cut in cuts[1:]:
        loudness = loudness * one(*cut)
    return loudness


def gaussian(stream_key, extent, scale, bound, cuts=(), kind=jnp.bfloat16):
    drawn = scale * jax.random.normal(stream_key, extent, jnp.float32)
    if cuts:
        drawn = drawn * shard_levels(stream_key, extent, cuts, -0.22, 0.18)
    return jnp.clip(drawn, -bound, bound).astype(kind)


def setup_inputs(seed: int = 0, part: int = 0) -> dict:
    key_list = jax.random.split(jax.random.key(seed), 9)
    part_keys = jax.random.split(jax.random.fold_in(key_list[8], part), 9)
    return {
        "volume": gaussian(part_keys[0], (NZ, SIDE, SIDE), 1.0, 6.0, ((0, 4), (1, 2), (2, 2)), jnp.float32),
        "tile_table": gaussian(key_list[1], (NTILES, TILE, TILE), (SLOTS * TILE) ** -0.5, 0.09375),
        "tile_ids": place_ends(jax.random.randint(key_list[2], (SLABS, COLS, HALVES, ANGLES, SLOTS), 0, NTILES), jax.random.fold_in(key_list[2], 1), 0, NTILES - 1).astype(jnp.int32),
        "block_ids": place_ends(jax.random.randint(key_list[3], (SLABS, COLS, HALVES, ANGLES, SLOTS * WIN * UBLK), 0, NBLK), jax.random.fold_in(key_list[3], 1), 0, NBLK - 1).astype(jnp.int32),
        "live_slots": draw_live_slots(jax.random.fold_in(key_list[8], 71), part),
        "measured": gaussian(part_keys[5], (ANGLES, DET_U, NZ), 2.0, 12.0, ((0, 4), (1, 4)), jnp.float32),
        "row_norm": jnp.clip(jnp.exp(math.log(1.0) - 1.609438 * jax.random.uniform(key_list[6], (ANGLES, DET_U, NZ), jnp.float32) ** shard_levels(key_list[6], (ANGLES, DET_U, NZ), ((0, 4), (1, 4)), -0.2, 0.2)), 0.2, 1.0),
        "col_norm": jnp.clip(jnp.exp(math.log(2.0) - 1.3862944 * jax.random.uniform(key_list[7], (NZ, SIDE, SIDE), jnp.float32) ** shard_levels(key_list[7], (NZ, SIDE, SIDE), ((0, 4), (1, 2), (2, 2)), -0.2, 0.2)), 0.5, 2.0),
    }


def reference(volume, tile_table, tile_ids, block_ids, live_slots, measured, row_norm, col_norm):
    piece_count = SLABS * COLS * HALVES
    pieces = volume.reshape(SLABS, SLAB_Z, COLS, XCOL, HALVES, YHALF).transpose(0, 2, 4, 1, 3, 5)
    voxel_rows = pieces.reshape(piece_count, NBLK, TILE).astype(jnp.bfloat16)
    tile_rows = tile_ids.reshape(piece_count, ANGLES, SLOTS)
    block_rows = block_ids.reshape(piece_count, ANGLES, SLOTS, WIN, UBLK)
    position = jnp.arange(SLOTS, dtype=jnp.int32)
    slot_mask = (position[None, None, :] < live_slots.reshape(piece_count, ANGLES)[:, :, None]).astype(jnp.float32)

    def forward(inputs):
        voxel_piece, tile_piece, block_piece, mask_piece = inputs
        picked = tile_table[tile_piece].astype(jnp.float32)
        voxels = voxel_piece[block_piece].astype(jnp.float32)
        return jnp.einsum("akdv,akwqv,ak->awqd", picked, voxels, mask_piece)

    partial_value = lax.map(forward, (voxel_rows, tile_rows, block_rows, slot_mask))
    per_slab = partial_value.reshape(SLABS, COLS * HALVES, ANGLES, WIN, DET_U).sum(axis=1)
    middle = per_slab[:, :, 1:SLAB_Z + 1]
    lower_rim = middle[:, :, 0].at[1:].add(per_slab[:-1, :, SLAB_Z + 1])
    upper_rim = middle[:, :, SLAB_Z - 1].at[:-1].add(per_slab[1:, :, 0])
    middle = middle.at[:, :, 0].set(lower_rim).at[:, :, SLAB_Z - 1].set(upper_rim)
    projection = middle.transpose(1, 3, 0, 2).reshape(ANGLES, DET_U, NZ)
    residual = (row_norm * (measured - projection)).astype(jnp.bfloat16)
    padded = jnp.pad(residual, ((0, 0), (0, 0), (1, 1)))
    head_rows = padded[:, :, :NZ].reshape(ANGLES, DET_U, SLABS, SLAB_Z)
    tail_rows = padded[:, :, 2:].reshape(ANGLES, DET_U, SLABS, SLAB_Z)[:, :, :, SLAB_Z - 2:]
    windows = jnp.concatenate([head_rows, tail_rows], axis=3).transpose(2, 0, 3, 1)
    windows = windows.reshape(SLABS, ANGLES, WIN, UBLK, TILE)
    piece_windows = jnp.repeat(windows, COLS * HALVES, axis=0)

    def backward(inputs):
        tile_piece, block_piece, mask_piece, window_piece = inputs
        picked = tile_table[tile_piece].astype(jnp.float32)
        spread = jnp.einsum("akdv,awqd,ak->akwqv", picked, window_piece.astype(jnp.float32), mask_piece)
        return jnp.zeros((NBLK, TILE), jnp.float32).at[block_piece].add(spread)

    back_sum = lax.map(backward, (tile_rows, block_rows, slot_mask, piece_windows))
    back_sum = back_sum.reshape(SLABS, COLS, HALVES, SLAB_Z, XCOL, YHALF).transpose(0, 3, 1, 4, 2, 5)
    return volume + col_norm * back_sum.reshape(NZ, SIDE, SIDE)
```

```python
import functools

import jax
import jax.numpy as jnp
from jax import lax
from jax.experimental import pallas as pl
from jax.experimental.pallas import tpu as pltpu
from jax.sharding import PartitionSpec as P

MESH = pl.DeviceIdType.MESH
F_UNROLL = 8
B_UNROLL = 4
ACCS = 4
OUT_PARTS = 4


def project_kernel(
    sizes,
    tid,
    blk,
    vol,
    table,
    meas,
    norm,
    res,
    tbl,
    vox,
    xs,
    acc,
    padw,
    sendw,
    recvw,
    tgt,
    part,
    peer,
    rim_lo,
    rim_hi,
    local_sem,
    wsend,
    wrecv,
    psend,
    precv,
    rsend,
    rrecv,
):
    nz, nx, nr = sizes
    pieces = nx * nr
    gz, gx, row = lax.axis_index("gz"), lax.axis_index("gx"), lax.axis_index("row")
    me = gx * nr + row
    angles, slots = tid.shape
    per_slot = blk.shape[1] // slots
    tiles, tile = table.shape[0], table.shape[1]
    rows, width = vol.shape
    runs = width // tile
    own_angles, cols, det_rows = meas.shape
    window = sendw.shape[3]
    depth = window - 2
    block_cols = per_slot // window
    groups, _, rim, _ = res.shape

    copies = [
        pltpu.make_async_copy(
            vol.at[:, pl.ds(h * tile, tile)], vox.at[pl.ds(h * rows, rows)], local_sem.at[h]
        )
        for h in range(runs)
    ]
    copies.append(pltpu.make_async_copy(table, tbl.at[pl.ds(0, tiles)], local_sem.at[runs]))
    for copy in copies:
        copy.start()

    barrier = pltpu.get_barrier_semaphore()
    others = [
        (dz, dx, dr)
        for dz in range(nz)
        for dx in range(nx)
        for dr in range(nr)
        if (dz, dx, dr) != (0, 0, 0)
    ]

    def at(dz, dx, dr):
        return {
            "gz": lax.rem(gz + dz, nz),
            "gx": lax.rem(gx + dx, nx),
            "row": lax.rem(row + dr, nr),
        }

    rim_lo[...] = jnp.zeros_like(rim_lo)
    rim_hi[...] = jnp.zeros_like(rim_hi)
    for offset in others:
        pl.semaphore_signal(barrier, inc=1, device_id=at(*offset), device_id_type=MESH)

    tbl[tiles] = jnp.zeros(tbl.shape[1:], tbl.dtype)
    acc[...] = jnp.zeros_like(acc)
    padw[...] = jnp.zeros_like(padw)
    for oa in range(own_angles):
        for j, ref in enumerate((meas, norm)):
            padw[j, 1 : det_rows + 1, :] = ref[oa].T
        for s in range(nz):
            for j in range(2):
                sendw[s, oa, j] = padw[j, s * depth : s * depth + window, :]
    recvw[gz, me] = sendw[gz]

    pl.semaphore_wait(barrier, len(others))
    windows = []
    for n, offset in enumerate(others):
        there = at(*offset)
        windows.append(
            pltpu.make_async_remote_copy(
                src_ref=sendw.at[there["gz"]],
                dst_ref=recvw.at[gz, me],
                send_sem=wsend.at[n],
                recv_sem=wrecv.at[n],
                device_id=there,
                device_id_type=MESH,
            )
        )
        windows[-1].start()

    for copy in copies:
        copy.wait()

    per_angle = slots // F_UNROLL
    steps = angles * per_angle

    def gather(step):
        a, k0 = step // per_angle, (step % per_angle) * F_UNROLL
        for j in range(F_UNROLL):
            for r in range(per_slot):
                at_row = blk[a, (k0 + j) * per_slot + r]
                xs[r : r + 1, j * tile : (j + 1) * tile] = vox[pl.ds(at_row, 1), :]

    def forward(step, carry):
        a, k0 = step // per_angle, (step % per_angle) * F_UNROLL
        x = xs[...].astype(jnp.bfloat16)
        t = jnp.concatenate([tbl[tid[a, k0 + j]] for j in range(F_UNROLL)], axis=1)
        d = lax.dot_general(x, t, (((1,), (1,)), ((), ())), preferred_element_type=jnp.float32)
        gather(jnp.minimum(step + 1, steps - 1))
        acc[a] += d
        return carry

    gather(jnp.int32(0))
    lax.fori_loop(0, steps, forward, 0)

    for g in range(groups):
        for a in range(angles):
            part[g, a] = acc[a, g * rim : (g + 1) * rim, :].astype(part.dtype)

    slab = [(dx, dr) for dx in range(nx) for dr in range(nr)]
    sends = []
    for n, (dx, dr) in enumerate(slab[1:]):
        sends.append(
            pltpu.make_async_remote_copy(
                src_ref=part,
                dst_ref=peer.at[n],
                send_sem=psend.at[n],
                recv_sem=precv.at[n],
                device_id=at(0, dx, dr),
                device_id_type=MESH,
            )
        )

    def rim_copy(up, n):
        dx, dr = slab[n]
        there = at(0, dx, dr)
        there["gz"] = jnp.minimum(gz + 1, nz - 1) if up else jnp.maximum(gz - 1, 0)
        return pltpu.make_async_remote_copy(
            src_ref=part.at[groups - 1 if up else 0],
            dst_ref=(rim_lo if up else rim_hi).at[n],
            send_sem=rsend.at[int(up), n],
            recv_sem=rrecv.at[int(up), n],
            device_id=there,
            device_id_type=MESH,
        )

    for copy in sends:
        copy.start()

    @pl.when(gz < nz - 1)
    def _():
        for n in range(pieces):
            rim_copy(True, n).start()

    @pl.when(gz > 0)
    def _():
        for n in range(pieces):
            rim_copy(False, n).start()

    for copy in windows:
        copy.wait()
    per_block = tile // cols
    for z in range(nz):
        for oa in range(own_angles):
            for j in range(2):
                for b in range(block_cols):
                    cut = [recvw[z, b * per_block + i, oa, j] for i in range(per_block)]
                    value = cut[0] if per_block == 1 else jnp.concatenate(cut, axis=1)
                    tgt[j, z * own_angles + oa, pl.ds(b, window, stride=block_cols), :] = value

    for copy in sends:
        copy.wait()

    @pl.when(gz < nz - 1)
    def _():
        for n in range(pieces):
            rim_copy(True, n).wait_send()
            rim_copy(False, n).wait_recv()

    @pl.when(gz > 0)
    def _():
        for n in range(pieces):
            rim_copy(False, n).wait_send()
            rim_copy(True, n).wait_recv()

    for g in range(groups):
        for a in range(angles):
            total = acc[a, g * rim : (g + 1) * rim, :]
            for n in range(pieces - 1):
                total = total + peer[n, g, a].astype(jnp.float32)
            if g == 0:
                for n in range(pieces):
                    total = total + rim_lo[n, a].astype(jnp.float32)
            if g == groups - 1:
                for n in range(pieces):
                    total = total + rim_hi[n, a].astype(jnp.float32)
            rows_in = slice(g * rim, (g + 1) * rim)
            value = tgt[1, a, rows_in, :] * (tgt[0, a, rows_in, :] - total)
            res[g, a] = value.astype(res.dtype)


def back_kernel(
    tid, blk, live, res, table, vol, norm, out, tbl, volv, normv, outv, rs, ss, todo, sem, out_sem,
    *accs
):
    angles, slots = tid.shape
    per_slot = blk.shape[1] // slots
    tiles, tile = table.shape[0], table.shape[1]
    rows, width = vol.shape
    runs = width // tile
    groups, _, rim, _ = res.shape
    copies = [
        pltpu.make_async_copy(table, tbl.at[pl.ds(0, tiles)], sem.at[0]),
        pltpu.make_async_copy(vol, volv, sem.at[1]),
        pltpu.make_async_copy(norm, normv, sem.at[2]),
    ]
    for copy in copies:
        copy.start()
    tbl[tiles] = jnp.zeros(tbl.shape[1:], tbl.dtype)
    per_angle = slots // B_UNROLL
    count = jnp.int32(0)
    for a in range(angles):
        need = (live[a] + B_UNROLL - 1) // B_UNROLL

        def put(i, c, a=a):
            todo[c] = a * per_angle + i
            return c + 1

        count = lax.fori_loop(0, need, put, count)
        rs[a] = jnp.concatenate([res[g, a].astype(jnp.float32) for g in range(groups)], axis=0)

    chunk = 64

    def clear(i, carry):
        for ref in accs:
            ref[pl.ds(pl.multiple_of(i * chunk, chunk), chunk), :] = jnp.zeros(
                (chunk, tile), jnp.float32
            )
        return carry

    lax.fori_loop(0, runs * rows // chunk, clear, 0)
    copies[0].wait()

    def spread(step):
        a, k0 = step // per_angle, (step % per_angle) * B_UNROLL
        t = jnp.concatenate([tbl[tid[a, k0 + j]] for j in range(B_UNROLL)], axis=1)
        return jnp.dot(rs[a].astype(jnp.bfloat16), t, preferred_element_type=jnp.float32)

    def back(i, carry):
        later = spread(todo[jnp.minimum(i + 1, count - 1)])
        step = todo[i]
        a, k0 = step // per_angle, (step % per_angle) * B_UNROLL
        for j in range(B_UNROLL):
            for r in range(per_slot):
                at_row = blk[a, (k0 + j) * per_slot + r]
                accs[r % ACCS][pl.ds(at_row, 1), :] += ss[r : r + 1, j * tile : (j + 1) * tile]
        ss[...] = later
        return carry

    ss[...] = spread(todo[0])
    lax.fori_loop(0, count, back, 0)

    copies[1].wait()
    copies[2].wait()
    size = rows // OUT_PARTS
    sub = 32
    outs = []
    for p in range(OUT_PARTS):

        def join(i, carry, p=p):
            first = pl.multiple_of(p * size + i * sub, sub)
            for h in range(runs):
                lanes = slice(h * tile, (h + 1) * tile)
                total = accs[0][pl.ds(h * rows + first, sub), :]
                for ref in accs[1:]:
                    total = total + ref[pl.ds(h * rows + first, sub), :]
                outv[pl.ds(first, sub), lanes] = (
                    volv[pl.ds(first, sub), lanes] + normv[pl.ds(first, sub), lanes] * total
                )
            return carry

        lax.fori_loop(0, size // sub, join, 0)
        part = pl.ds(p * size, size)
        outs.append(pltpu.make_async_copy(outv.at[part], out.at[part], out_sem.at[p]))
        outs[-1].start()
    for copy in outs:
        copy.wait()


def on_device(sizes, volume, tile_table, tile_ids, block_ids, live_slots, measured, row_norm, col_norm):
    nz, nx, nr = sizes
    pieces = nx * nr
    depth, column_width, half_width = volume.shape
    tiles, tile = tile_table.shape[0], tile_table.shape[1]
    angles, slots = tile_ids.shape[3], tile_ids.shape[4]
    window = depth + 2
    per_slot = block_ids.shape[4] // slots
    block_cols = per_slot // window
    rim = 2 * block_cols
    groups = window // 2
    runs = half_width // tile
    rows = depth * column_width
    own_angles, cols, det_rows = measured.shape
    vmem = pl.BlockSpec(memory_space=pltpu.VMEM)
    smem = pl.BlockSpec(memory_space=pltpu.SMEM)
    anyw = pl.BlockSpec(memory_space=pl.ANY)

    live = live_slots.reshape(angles)
    blocks = block_ids.reshape(angles, slots * per_slot)
    blk = (blocks % runs) * rows + blocks // runs
    position = jnp.arange(slots, dtype=jnp.int32)
    tid = jnp.where(position[None, :] < live[:, None], tile_ids.reshape(angles, slots), tiles)
    vol = volume.reshape(rows, half_width)
    norm = col_norm.reshape(rows, half_width)
    n_others = nz * pieces - 1
    n_peers = max(pieces - 1, 1)
    dma = pltpu.SemaphoreType.DMA
    f32, bf16 = jnp.float32, jnp.bfloat16

    res = pl.pallas_call(
        functools.partial(project_kernel, sizes),
        out_shape=jax.ShapeDtypeStruct((groups, angles, rim, tile), bf16),
        in_specs=[smem, smem, anyw, anyw, vmem, vmem],
        out_specs=vmem,
        scratch_shapes=[
            pltpu.VMEM((tiles + 1, tile, tile), tile_table.dtype),
            pltpu.VMEM((runs * rows, tile), f32),
            pltpu.VMEM((per_slot, F_UNROLL * tile), f32),
            pltpu.VMEM((angles, per_slot, tile), f32),
            pltpu.VMEM((2, det_rows + 2, cols), f32),
            pltpu.VMEM((nz, own_angles, 2, window, cols), f32),
            pltpu.VMEM((nz, pieces, own_angles, 2, window, cols), f32),
            pltpu.VMEM((2, angles, per_slot, tile), f32),
            pltpu.VMEM((groups, angles, rim, tile), bf16),
            pltpu.VMEM((n_peers, groups, angles, rim, tile), bf16),
            pltpu.VMEM((pieces, angles, rim, tile), bf16),
            pltpu.VMEM((pieces, angles, rim, tile), bf16),
            dma((runs + 1,)),
            dma((n_others,)),
            dma((n_others,)),
            dma((n_peers,)),
            dma((n_peers,)),
            dma((2, pieces)),
            dma((2, pieces)),
        ],
        compiler_params=pltpu.CompilerParams(
            collective_id=0, has_side_effects=True, vmem_limit_bytes=24 << 20
        ),
        name="project",
    )(tid, blk, vol, tile_table, measured, row_norm)

    out = pl.pallas_call(
        back_kernel,
        out_shape=jax.ShapeDtypeStruct((rows, half_width), f32),
        in_specs=[smem, smem, smem, vmem, anyw, anyw, anyw],
        out_specs=anyw,
        scratch_shapes=[
            pltpu.VMEM((tiles + 1, tile, tile), tile_table.dtype),
            pltpu.VMEM((rows, half_width), f32),
            pltpu.VMEM((rows, half_width), f32),
            pltpu.VMEM((rows, half_width), f32),
            pltpu.VMEM((angles, per_slot, tile), f32),
            pltpu.VMEM((per_slot, B_UNROLL * tile), f32),
            pltpu.SMEM((angles * slots // B_UNROLL,), jnp.int32),
            dma((3,)),
            dma((OUT_PARTS,)),
        ]
        + [pltpu.VMEM((runs * rows, tile), f32)] * ACCS,
        compiler_params=pltpu.CompilerParams(vmem_limit_bytes=32 << 20),
        name="spread_back",
    )(tid, blk, live, res, tile_table, vol, norm)
    return out.reshape(volume.shape)


def solution(mesh):
    placed = (
        P(("grp", "gz"), "gx", "row"),
        P(),
        P("gz", "gx", "row", None, None),
        P("gz", "gx", "row", None, None),
        P("gz", "gx", "row", None),
        P(("grp", "gz"), ("gx", "row"), None),
        P("gz", ("gx", "row"), None),
        P("gz", "gx", "row"),
    )
    sizes = (mesh.shape["gz"], mesh.shape["gx"], mesh.shape["row"])
    return jax.shard_map(
        functools.partial(on_device, sizes),
        mesh=mesh,
        in_specs=placed,
        out_specs=P(("grp", "gz"), "gx", "row"),
        check_vma=False,
    )
```

```python
import functools

import jax
import jax.numpy as jnp
from jax import lax
from jax.experimental import pallas as pl
from jax.experimental.pallas import tpu as pltpu
from jax.sharding import PartitionSpec as P

MESH = pl.DeviceIdType.MESH
F_UNROLL = 8
B_UNROLL = 4
ACCS = 4
OUT_PARTS = 4
VMEM = 67043328


def project_kernel(
    sizes,
    tid,
    live,
    blocks,
    vol,
    table,
    meas,
    norm,
    res,
    blk,
    tbl,
    vox,
    xs,
    acc,
    padw,
    sendw,
    recvw,
    tgt,
    part,
    peer,
    rim_lo,
    rim_hi,
    local_sem,
    wsend,
    wrecv,
    psend,
    precv,
    rsend,
    rrecv,
):
    nz, nx, nr = sizes
    pieces = nx * nr
    gz, gx, row = lax.axis_index("gz"), lax.axis_index("gx"), lax.axis_index("row")
    me = gx * nr + row
    angles, slots = tid.shape
    per_slot = blocks.shape[1] // slots
    tile = table.shape[1]
    rows, width = vol.shape
    runs = width // tile
    own_angles, det_rows, cols = meas.shape
    window = sendw.shape[3]
    depth = window - 2
    block_cols = per_slot // window
    groups, _, rim, _ = res.shape

    copies = index_copies(blocks, blk, local_sem, runs + 1)
    by_run = vox.reshape(rows, runs, 1, tile)
    copies += [
        pltpu.make_async_copy(
            vol.at[:, pl.ds(h * tile, tile)], by_run.at[:, h, 0], local_sem.at[h]
        )
        for h in range(runs)
    ]
    copies.append(pltpu.make_async_copy(table, tbl, local_sem.at[runs]))
    for copy in copies:
        copy.start()

    barrier = pltpu.get_barrier_semaphore()
    others = [
        (dz, dx, dr)
        for dz in range(nz)
        for dx in range(nx)
        for dr in range(nr)
        if (dz, dx, dr) != (0, 0, 0)
    ]

    def at(dz, dx, dr):
        return {
            "gz": lax.rem(gz + dz, nz),
            "gx": lax.rem(gx + dx, nx),
            "row": lax.rem(row + dr, nr),
        }

    rim_lo[...] = jnp.zeros_like(rim_lo)
    rim_hi[...] = jnp.zeros_like(rim_hi)
    for offset in others:
        pl.semaphore_signal(barrier, inc=1, device_id=at(*offset), device_id_type=MESH)

    acc[...] = jnp.zeros_like(acc)
    padw[...] = jnp.zeros_like(padw)
    for oa in range(own_angles):
        for j, ref in enumerate((meas, norm)):
            padw[j, 1 : det_rows + 1, :] = ref[oa]
        for s in range(nz):
            for j in range(2):
                sendw[s, oa, j] = padw[j, s * depth : s * depth + window, :]
    recvw[gz, me] = sendw[gz]

    pl.semaphore_wait(barrier, len(others))
    windows = []
    for n, offset in enumerate(others):
        there = at(*offset)
        windows.append(
            pltpu.make_async_remote_copy(
                src_ref=sendw.at[there["gz"]],
                dst_ref=recvw.at[gz, me],
                send_sem=wsend.at[n],
                recv_sem=wrecv.at[n],
                device_id=there,
                device_id_type=MESH,
            )
        )
        windows[-1].start()

    for copy in copies:
        copy.wait()

    per_angle = slots // F_UNROLL
    steps = angles * per_angle

    def gather(step):
        first = step * (F_UNROLL * per_slot)
        for j in range(F_UNROLL):
            for r in range(per_slot):
                at_row = blk[first + (j * per_slot + r)]
                xs[r : r + 1, j * tile : (j + 1) * tile] = vox[at_row]

    def forward(step, carry):
        a, k0 = step // per_angle, (step % per_angle) * F_UNROLL
        x = xs[...].astype(jnp.bfloat16)
        t = live_tiles(tbl, tid, live, a, k0, F_UNROLL)
        d = lax.dot_general(x, t, (((1,), (1,)), ((), ())), preferred_element_type=jnp.float32)
        gather(jnp.minimum(step + 1, steps - 1))
        acc[a] += d
        return carry

    gather(jnp.int32(0))
    lax.fori_loop(0, steps, forward, 0)

    for g in range(groups):
        for a in range(angles):
            part[g, a] = acc[a, g * rim : (g + 1) * rim, :].astype(part.dtype)

    slab = [(dx, dr) for dx in range(nx) for dr in range(nr)]
    sends = []
    for n, (dx, dr) in enumerate(slab[1:]):
        sends.append(
            pltpu.make_async_remote_copy(
                src_ref=part,
                dst_ref=peer.at[n],
                send_sem=psend.at[n],
                recv_sem=precv.at[n],
                device_id=at(0, dx, dr),
                device_id_type=MESH,
            )
        )

    def rim_copy(up, n):
        dx, dr = slab[n]
        there = at(0, dx, dr)
        there["gz"] = jnp.minimum(gz + 1, nz - 1) if up else jnp.maximum(gz - 1, 0)
        return pltpu.make_async_remote_copy(
            src_ref=part.at[groups - 1 if up else 0],
            dst_ref=(rim_lo if up else rim_hi).at[n],
            send_sem=rsend.at[int(up), n],
            recv_sem=rrecv.at[int(up), n],
            device_id=there,
            device_id_type=MESH,
        )

    for copy in sends:
        copy.start()

    @pl.when(gz < nz - 1)
    def _():
        for n in range(pieces):
            rim_copy(True, n).start()

    @pl.when(gz > 0)
    def _():
        for n in range(pieces):
            rim_copy(False, n).start()

    for copy in windows:
        copy.wait()
    per_block = tile // cols
    for z in range(nz):
        for oa in range(own_angles):
            for j in range(2):
                for b in range(block_cols):
                    cut = [recvw[z, b * per_block + i, oa, j] for i in range(per_block)]
                    value = cut[0] if per_block == 1 else jnp.concatenate(cut, axis=1)
                    tgt[j, z * own_angles + oa, pl.ds(b, window, stride=block_cols), :] = value

    for copy in sends:
        copy.wait()

    @pl.when(gz < nz - 1)
    def _():
        for n in range(pieces):
            rim_copy(True, n).wait_send()
            rim_copy(False, n).wait_recv()

    @pl.when(gz > 0)
    def _():
        for n in range(pieces):
            rim_copy(False, n).wait_send()
            rim_copy(True, n).wait_recv()

    for g in range(groups):
        for a in range(angles):
            total = acc[a, g * rim : (g + 1) * rim, :]
            for n in range(pieces - 1):
                total = total + peer[n, g, a].astype(jnp.float32)
            if g == 0:
                for n in range(pieces):
                    total = total + rim_lo[n, a].astype(jnp.float32)
            if g == groups - 1:
                for n in range(pieces):
                    total = total + rim_hi[n, a].astype(jnp.float32)
            rows_in = slice(g * rim, (g + 1) * rim)
            value = tgt[1, a, rows_in, :] * (tgt[0, a, rows_in, :] - total)
            res[g, a] = value.astype(res.dtype)


def index_copies(blocks, blk, sem, base):
    angles, length = blocks.shape
    return [
        pltpu.make_async_copy(blocks.at[a], blk.at[pl.ds(a * length, length)], sem.at[base + a])
        for a in range(angles)
    ]


def live_tiles(tbl, tid, live, a, k0, count):
    tiles = []
    for j in range(count):
        picked = tbl[tid[a, k0 + j]]
        tiles.append(jnp.where(k0 + j < live[a], picked, jnp.zeros_like(picked)))
    return jnp.concatenate(tiles, axis=1)


def back_kernel(
    tid, live, blocks, res, table, vol, norm, out, blk, tbl, volv, normv, outv, rs, ss, todo, sem, out_sem,
    *accs
):
    angles, slots = tid.shape
    per_slot = blocks.shape[1] // slots
    tile = tbl.shape[1]
    rows, width = vol.shape
    runs = width // tile
    groups, _, rim, _ = res.shape
    indices = index_copies(blocks, blk, sem, 3)
    indices.append(pltpu.make_async_copy(table, tbl, sem.at[2]))
    copies = [
        pltpu.make_async_copy(vol, volv, sem.at[0]),
        pltpu.make_async_copy(norm, normv, sem.at[1]),
    ]
    for copy in indices + copies:
        copy.start()
    per_angle = slots // B_UNROLL
    count = jnp.int32(0)
    for a in range(angles):
        need = (live[a] + B_UNROLL - 1) // B_UNROLL

        def put(i, c, a=a):
            todo[c] = a * per_angle + i
            return c + 1

        count = lax.fori_loop(0, need, put, count)
        rs[a] = jnp.concatenate([res[g, a].astype(jnp.float32) for g in range(groups)], axis=0)

    chunk = 64

    def clear(i, carry):
        for ref in accs:
            ref[pl.ds(pl.multiple_of(i * chunk, chunk), chunk), :] = jnp.zeros(
                (chunk, tile), jnp.float32
            )
        return carry

    lax.fori_loop(0, runs * rows // chunk, clear, 0)
    for copy in indices:
        copy.wait()

    def spread(step):
        a, k0 = step // per_angle, (step % per_angle) * B_UNROLL
        t = live_tiles(tbl, tid, live, a, k0, B_UNROLL)
        return jnp.dot(rs[a].astype(jnp.bfloat16), t, preferred_element_type=jnp.float32)

    def back(i, carry):
        later = spread(todo[jnp.maximum(jnp.minimum(i + 1, count - 1), 0)])
        first = todo[i] * (B_UNROLL * per_slot)
        for j in range(B_UNROLL):
            for r in range(per_slot):
                at_row = blk[first + (j * per_slot + r)]
                accs[r % ACCS][pl.ds(at_row, 1), :] += ss[r : r + 1, j * tile : (j + 1) * tile]
        ss[...] = later
        return carry

    ss[...] = spread(todo[0])
    lax.fori_loop(0, count, back, 0)

    for copy in copies:
        copy.wait()
    size = rows // OUT_PARTS
    sub = 32
    outs = []
    for p in range(OUT_PARTS):

        def join(i, carry, p=p):
            first = pl.multiple_of(p * size + i * sub, sub)
            for h in range(runs):
                lanes = slice(h * tile, (h + 1) * tile)
                part = pl.ds(pl.multiple_of(first * runs, sub * runs), sub * runs)
                lane = pl.ds(h, sub, stride=runs)
                total = accs[0].at[part][lane, :]
                for ref in accs[1:]:
                    total = total + ref.at[part][lane, :]
                outv[pl.ds(first, sub), lanes] = (
                    volv[pl.ds(first, sub), lanes] + normv[pl.ds(first, sub), lanes] * total
                )
            return carry

        lax.fori_loop(0, size // sub, join, 0)
        part = pl.ds(p * size, size)
        outs.append(pltpu.make_async_copy(outv.at[part], out.at[part], out_sem.at[p]))
        outs[-1].start()
    for copy in outs:
        copy.wait()


def on_device(sizes, volume, tile_table, tile_ids, block_ids, live_slots, measured, row_norm, col_norm):
    nz, nx, nr = sizes
    pieces = nx * nr
    depth, column_width, half_width = volume.shape
    tile = tile_table.shape[1]
    angles, slots = tile_ids.shape[3], tile_ids.shape[4]
    window = depth + 2
    per_slot = block_ids.shape[4] // slots
    block_cols = per_slot // window
    rim = 2 * block_cols
    groups = window // 2
    runs = half_width // tile
    rows = depth * column_width
    measured = measured.transpose(0, 2, 1)
    row_norm = row_norm.transpose(0, 2, 1)
    own_angles, det_rows, cols = measured.shape
    vmem = pl.BlockSpec(memory_space=pltpu.VMEM)
    smem = pl.BlockSpec(memory_space=pltpu.SMEM)
    hbm = pl.BlockSpec(memory_space=pltpu.HBM)

    live = live_slots.reshape(angles)
    blocks = block_ids.reshape(angles, slots * per_slot)
    tid = tile_ids.reshape(angles, slots)
    index = pltpu.SMEM((angles * slots * per_slot,), jnp.int32)
    vol = volume.reshape(rows, half_width)
    norm = col_norm.reshape(rows, half_width)
    n_others = nz * pieces - 1
    n_peers = max(pieces - 1, 1)
    dma = pltpu.SemaphoreType.DMA
    f32, bf16 = jnp.float32, jnp.bfloat16

    res = pl.pallas_call(
        functools.partial(project_kernel, sizes),
        out_shape=jax.ShapeDtypeStruct((groups, angles, rim, tile), bf16),
        in_specs=[smem, smem, hbm, hbm, hbm, vmem, vmem],
        out_specs=vmem,
        scratch_shapes=[
            index,
            pltpu.VMEM(tile_table.shape, tile_table.dtype),
            pltpu.VMEM((rows * runs, 1, tile), f32),
            pltpu.VMEM((per_slot, F_UNROLL * tile), f32),
            pltpu.VMEM((angles, per_slot, tile), f32),
            pltpu.VMEM((2, det_rows + 2, cols), f32),
            pltpu.VMEM((nz, own_angles, 2, window, cols), f32),
            pltpu.VMEM((nz, pieces, own_angles, 2, window, cols), f32),
            pltpu.VMEM((2, angles, per_slot, tile), f32),
            pltpu.VMEM((groups, angles, rim, tile), bf16),
            pltpu.VMEM((n_peers, groups, angles, rim, tile), bf16),
            pltpu.VMEM((pieces, angles, rim, tile), bf16),
            pltpu.VMEM((pieces, angles, rim, tile), bf16),
            dma((runs + 1 + angles,)),
            dma((n_others,)),
            dma((n_others,)),
            dma((n_peers,)),
            dma((n_peers,)),
            dma((2, pieces)),
            dma((2, pieces)),
        ],
        compiler_params=pltpu.CompilerParams(
            collective_id=0, has_side_effects=True, vmem_limit_bytes=VMEM
        ),
        name="project",
    )(tid, live, blocks, vol, tile_table, measured, row_norm)

    out = pl.pallas_call(
        back_kernel,
        out_shape=jax.ShapeDtypeStruct((rows, half_width), f32),
        in_specs=[smem, smem, hbm, vmem, hbm, hbm, hbm],
        out_specs=hbm,
        scratch_shapes=[
            index,
            pltpu.VMEM(tile_table.shape, tile_table.dtype),
            pltpu.VMEM((rows, half_width), f32),
            pltpu.VMEM((rows, half_width), f32),
            pltpu.VMEM((rows, half_width), f32),
            pltpu.VMEM((angles, per_slot, tile), f32),
            pltpu.VMEM((per_slot, B_UNROLL * tile), f32),
            pltpu.SMEM((angles * slots // B_UNROLL,), jnp.int32),
            dma((3 + angles,)),
            dma((OUT_PARTS,)),
        ]
        + [pltpu.VMEM((runs * rows, tile), f32)] * ACCS,
        compiler_params=pltpu.CompilerParams(vmem_limit_bytes=VMEM),
        name="spread_back",
    )(tid, live, blocks, res, tile_table, vol, norm)
    return out.reshape(volume.shape)


def solution(mesh):
    placed = (
        P(("grp", "gz"), "gx", "row"),
        P(),
        P("gz", "gx", "row", None, None),
        P("gz", "gx", "row", None, None),
        P("gz", "gx", "row", None),
        P(("grp", "gz"), ("gx", "row"), None),
        P("gz", ("gx", "row"), None),
        P("gz", "gx", "row"),
    )
    sizes = (mesh.shape["gz"], mesh.shape["gx"], mesh.shape["row"])
    return jax.shard_map(
        functools.partial(on_device, sizes),
        mesh=mesh,
        in_specs=placed,
        out_specs=P(("grp", "gz"), "gx", "row"),
        check_vma=False,
    )
```

```python
import functools

import jax
import jax.numpy as jnp
from jax import lax
from jax.experimental import pallas as pl
from jax.experimental.pallas import tpu as pltpu
from jax.sharding import PartitionSpec as P

MESH = pl.DeviceIdType.MESH
F_UNROLL = 8
B_UNROLL = 4
ACCS = 4
OUT_PARTS = 4
VMEM = 67043328


def project_kernel(
    sizes,
    tid_hbm,
    live_hbm,
    blocks,
    vol,
    table,
    meas_hbm,
    norm_hbm,
    res,
    tid,
    live,
    meas,
    norm,
    blk,
    tbl,
    vox,
    xs,
    acc,
    padw,
    sendw,
    recvw,
    tgt,
    part,
    peer,
    rim_lo,
    rim_hi,
    local_sem,
    wsend,
    wrecv,
    psend,
    precv,
    rsend,
    rrecv,
):
    nz, nx, nr = sizes
    pieces = nx * nr
    gz, gx, row = lax.axis_index("gz"), lax.axis_index("gx"), lax.axis_index("row")
    me = gx * nr + row
    angles, slots = tid.shape
    per_slot = blocks.shape[1] // slots
    tile = table.shape[1]
    rows, width = vol.shape
    runs = width // tile
    own_angles, det_rows, cols = meas.shape
    window = sendw.shape[3]
    depth = window - 2
    block_cols = per_slot // window
    groups, _, rim, _ = res.shape

    by_run = vox.reshape(rows, runs, 1, tile)
    small = [
        pltpu.make_async_copy(meas_hbm, meas, local_sem.at[runs + 1]),
        pltpu.make_async_copy(norm_hbm, norm, local_sem.at[runs + 2]),
    ]
    copies = [
        pltpu.make_async_copy(
            vol.at[:, pl.ds(h * tile, tile)], by_run.at[:, h, 0], local_sem.at[h]
        )
        for h in range(runs)
    ]
    copies.append(pltpu.make_async_copy(table, tbl, local_sem.at[runs]))
    copies += index_copies(blocks, blk, local_sem, runs + 5)
    copies.append(pltpu.make_async_copy(tid_hbm, tid, local_sem.at[runs + 3]))
    copies.append(pltpu.make_async_copy(live_hbm, live, local_sem.at[runs + 4]))
    for copy in small + copies:
        copy.start()

    barrier = pltpu.get_barrier_semaphore()
    others = [
        (dz, dx, dr)
        for dz in range(nz)
        for dx in range(nx)
        for dr in range(nr)
        if (dz, dx, dr) != (0, 0, 0)
    ]

    def at(dz, dx, dr):
        return {
            "gz": lax.rem(gz + dz, nz),
            "gx": lax.rem(gx + dx, nx),
            "row": lax.rem(row + dr, nr),
        }

    rim_lo[...] = jnp.zeros_like(rim_lo)
    rim_hi[...] = jnp.zeros_like(rim_hi)
    for offset in others:
        pl.semaphore_signal(barrier, inc=1, device_id=at(*offset), device_id_type=MESH)

    acc[...] = jnp.zeros_like(acc)
    padw[...] = jnp.zeros_like(padw)
    for copy in small:
        copy.wait()
    for oa in range(own_angles):
        for j, ref in enumerate((meas, norm)):
            padw[j, 1 : det_rows + 1, :] = ref[oa]
        for s in range(nz):
            for j in range(2):
                sendw[s, oa, j] = padw[j, s * depth : s * depth + window, :]
    recvw[gz, me] = sendw[gz]

    for copy in copies:
        copy.wait()

    per_angle = slots // F_UNROLL
    steps = angles * per_angle

    def gather(step):
        first = step * (F_UNROLL * per_slot)
        for j in range(F_UNROLL):
            for r in range(per_slot):
                at_row = blk[first + (j * per_slot + r)]
                xs[r : r + 1, j * tile : (j + 1) * tile] = vox[at_row]

    def forward(step, carry):
        a, k0 = step // per_angle, (step % per_angle) * F_UNROLL
        x = xs[...].astype(jnp.bfloat16)
        t = live_tiles(tbl, tid, live, a, k0, F_UNROLL)
        d = lax.dot_general(x, t, (((1,), (1,)), ((), ())), preferred_element_type=jnp.float32)
        gather(jnp.minimum(step + 1, steps - 1))
        acc[a] += d
        return carry

    slab = [(dx, dr) for dx in range(nx) for dr in range(nr)]
    early = max(3 * angles // 4, 1)
    spans = [(0, early)] + ([(early, angles - early)] if early < angles else [])

    def peer_copy(phase, n):
        span = pl.ds(*spans[phase])
        return pltpu.make_async_remote_copy(
            src_ref=part.at[:, span],
            dst_ref=peer.at[n - 1, :, span],
            send_sem=psend.at[phase, n - 1],
            recv_sem=precv.at[phase, n - 1],
            device_id=at(0, *slab[n]),
            device_id_type=MESH,
        )

    def rim_copy(phase, up, n):
        span = pl.ds(*spans[phase])
        there = at(0, *slab[n])
        there["gz"] = jnp.minimum(gz + 1, nz - 1) if up else jnp.maximum(gz - 1, 0)
        return pltpu.make_async_remote_copy(
            src_ref=part.at[groups - 1 if up else 0, span],
            dst_ref=(rim_lo if up else rim_hi).at[n, span],
            send_sem=rsend.at[phase, int(up), n],
            recv_sem=rrecv.at[phase, int(up), n],
            device_id=there,
            device_id_type=MESH,
        )

    def send(phase):
        first, count = spans[phase]
        for g in range(groups):
            for a in range(first, first + count):
                part[g, a] = acc[a, g * rim : (g + 1) * rim, :].astype(part.dtype)
        for n in range(1, pieces):
            peer_copy(phase, n).start()

        @pl.when(gz < nz - 1)
        def _():
            for n in range(pieces):
                rim_copy(phase, True, n).start()

        @pl.when(gz > 0)
        def _():
            for n in range(pieces):
                rim_copy(phase, False, n).start()

    gather(jnp.int32(0))
    lax.fori_loop(0, early * per_angle, forward, 0)
    pl.semaphore_wait(barrier, len(others))
    windows = []
    for n, offset in enumerate(others):
        there = at(*offset)
        windows.append(
            pltpu.make_async_remote_copy(
                src_ref=sendw.at[there["gz"]],
                dst_ref=recvw.at[gz, me],
                send_sem=wsend.at[n],
                recv_sem=wrecv.at[n],
                device_id=there,
                device_id_type=MESH,
            )
        )
        windows[-1].start()
    send(0)
    if len(spans) > 1:
        lax.fori_loop(early * per_angle, steps, forward, 0)
        send(1)

    for copy in windows:
        copy.wait()
    per_block = tile // cols
    for z in range(nz):
        for oa in range(own_angles):
            for j in range(2):
                for b in range(block_cols):
                    cut = [recvw[z, b * per_block + i, oa, j] for i in range(per_block)]
                    value = cut[0] if per_block == 1 else jnp.concatenate(cut, axis=1)
                    tgt[j, z * own_angles + oa, pl.ds(b, window, stride=block_cols), :] = value

    for phase in range(len(spans)):
        for n in range(1, pieces):
            peer_copy(phase, n).wait()

    @pl.when(gz < nz - 1)
    def _():
        for phase in range(len(spans)):
            for n in range(pieces):
                rim_copy(phase, True, n).wait_send()
                rim_copy(phase, False, n).wait_recv()

    @pl.when(gz > 0)
    def _():
        for phase in range(len(spans)):
            for n in range(pieces):
                rim_copy(phase, False, n).wait_send()
                rim_copy(phase, True, n).wait_recv()

    for g in range(groups):
        for a in range(angles):
            total = acc[a, g * rim : (g + 1) * rim, :]
            for n in range(pieces - 1):
                total = total + peer[n, g, a].astype(jnp.float32)
            if g == 0:
                for n in range(pieces):
                    total = total + rim_lo[n, a].astype(jnp.float32)
            if g == groups - 1:
                for n in range(pieces):
                    total = total + rim_hi[n, a].astype(jnp.float32)
            rows_in = slice(g * rim, (g + 1) * rim)
            value = tgt[1, a, rows_in, :] * (tgt[0, a, rows_in, :] - total)
            res[g, a] = value.astype(res.dtype)


def index_copies(blocks, blk, sem, base):
    angles, length = blocks.shape
    return [
        pltpu.make_async_copy(blocks.at[a], blk.at[pl.ds(a * length, length)], sem.at[base + a])
        for a in range(angles)
    ]


def live_tiles(tbl, tid, live, a, k0, count):
    tiles = []
    for j in range(count):
        picked = tbl[tid[a, k0 + j]]
        tiles.append(jnp.where(k0 + j < live[a], picked, jnp.zeros_like(picked)))
    return jnp.concatenate(tiles, axis=1)


def back_kernel(
    tid_hbm, live_hbm, blocks, res_hbm, table, vol, norm, out, tid, live, res, blk, tbl, volv,
    normv, outv, rs, ss, todo, sem, out_sem, *accs
):
    angles, slots = tid.shape
    per_slot = blocks.shape[1] // slots
    tile = tbl.shape[1]
    rows, width = vol.shape
    runs = width // tile
    groups, _, rim, _ = res.shape
    small = [
        pltpu.make_async_copy(live_hbm, live, sem.at[3]),
        pltpu.make_async_copy(res_hbm, res, sem.at[4]),
    ]
    indices = [pltpu.make_async_copy(table, tbl, sem.at[2])]
    indices.append(pltpu.make_async_copy(tid_hbm, tid, sem.at[5]))
    indices += index_copies(blocks, blk, sem, 6)
    copies = [
        pltpu.make_async_copy(vol, volv, sem.at[0]),
        pltpu.make_async_copy(norm, normv, sem.at[1]),
    ]
    for copy in small + indices:
        copy.start()
    chunk = 64

    def clear(i, carry):
        for ref in accs:
            ref[pl.ds(pl.multiple_of(i * chunk, chunk), chunk), :] = jnp.zeros(
                (chunk, tile), jnp.float32
            )
        return carry

    lax.fori_loop(0, runs * rows // chunk, clear, 0)
    for copy in small:
        copy.wait()
    per_angle = slots // B_UNROLL
    count = jnp.int32(0)
    for a in range(angles):
        need = (live[a] + B_UNROLL - 1) // B_UNROLL

        def put(i, c, a=a):
            todo[c] = a * per_angle + i
            return c + 1

        count = lax.fori_loop(0, need, put, count)
        rs[a] = jnp.concatenate([res[g, a].astype(jnp.float32) for g in range(groups)], axis=0)

    for copy in indices:
        copy.wait()
    for copy in copies:
        copy.start()

    def spread(step):
        a, k0 = step // per_angle, (step % per_angle) * B_UNROLL
        t = live_tiles(tbl, tid, live, a, k0, B_UNROLL)
        return jnp.dot(rs[a].astype(jnp.bfloat16), t, preferred_element_type=jnp.float32)

    def back(i, carry):
        later = spread(todo[jnp.maximum(jnp.minimum(i + 1, count - 1), 0)])
        first = todo[i] * (B_UNROLL * per_slot)
        for j in range(B_UNROLL):
            for r in range(per_slot):
                at_row = blk[first + (j * per_slot + r)]
                accs[r % ACCS][pl.ds(at_row, 1), :] += ss[r : r + 1, j * tile : (j + 1) * tile]
        ss[...] = later
        return carry

    ss[...] = spread(todo[0])
    lax.fori_loop(0, count, back, 0)

    for copy in copies:
        copy.wait()
    size = rows // OUT_PARTS
    sub = 32
    outs = []
    for p in range(OUT_PARTS):

        def join(i, carry, p=p):
            first = pl.multiple_of(p * size + i * sub, sub)
            for h in range(runs):
                lanes = slice(h * tile, (h + 1) * tile)
                part = pl.ds(pl.multiple_of(first * runs, sub * runs), sub * runs)
                lane = pl.ds(h, sub, stride=runs)
                total = accs[0].at[part][lane, :]
                for ref in accs[1:]:
                    total = total + ref.at[part][lane, :]
                outv[pl.ds(first, sub), lanes] = (
                    volv[pl.ds(first, sub), lanes] + normv[pl.ds(first, sub), lanes] * total
                )
            return carry

        lax.fori_loop(0, size // sub, join, 0)
        part = pl.ds(p * size, size)
        outs.append(pltpu.make_async_copy(outv.at[part], out.at[part], out_sem.at[p]))
        outs[-1].start()
    for copy in outs:
        copy.wait()


def on_device(sizes, volume, tile_table, tile_ids, block_ids, live_slots, measured, row_norm, col_norm):
    nz, nx, nr = sizes
    pieces = nx * nr
    depth, column_width, half_width = volume.shape
    tile = tile_table.shape[1]
    angles, slots = tile_ids.shape[3], tile_ids.shape[4]
    window = depth + 2
    per_slot = block_ids.shape[4] // slots
    block_cols = per_slot // window
    rim = 2 * block_cols
    groups = window // 2
    runs = half_width // tile
    rows = depth * column_width
    measured = measured.transpose(0, 2, 1)
    row_norm = row_norm.transpose(0, 2, 1)
    own_angles, det_rows, cols = measured.shape
    vmem = pl.BlockSpec(memory_space=pltpu.VMEM)
    hbm = pl.BlockSpec(memory_space=pltpu.HBM)

    live = live_slots.reshape(angles)
    blocks = block_ids.reshape(angles, slots * per_slot)
    tid = tile_ids.reshape(angles, slots)
    index = pltpu.SMEM((angles * slots * per_slot,), jnp.int32)
    chosen = pltpu.SMEM((angles, slots), jnp.int32)
    counts = pltpu.SMEM((angles,), jnp.int32)
    vol = volume.reshape(rows, half_width)
    norm = col_norm.reshape(rows, half_width)
    n_others = nz * pieces - 1
    n_peers = max(pieces - 1, 1)
    dma = pltpu.SemaphoreType.DMA
    f32, bf16 = jnp.float32, jnp.bfloat16

    res = pl.pallas_call(
        functools.partial(project_kernel, sizes),
        out_shape=jax.ShapeDtypeStruct((groups, angles, rim, tile), bf16),
        in_specs=[hbm] * 7,
        out_specs=vmem,
        scratch_shapes=[
            chosen,
            counts,
            pltpu.VMEM(measured.shape, f32),
            pltpu.VMEM(measured.shape, f32),
            index,
            pltpu.VMEM(tile_table.shape, tile_table.dtype),
            pltpu.VMEM((rows * runs, 1, tile), f32),
            pltpu.VMEM((per_slot, F_UNROLL * tile), f32),
            pltpu.VMEM((angles, per_slot, tile), f32),
            pltpu.VMEM((2, det_rows + 2, cols), f32),
            pltpu.VMEM((nz, own_angles, 2, window, cols), f32),
            pltpu.VMEM((nz, pieces, own_angles, 2, window, cols), f32),
            pltpu.VMEM((2, angles, per_slot, tile), f32),
            pltpu.VMEM((groups, angles, rim, tile), bf16),
            pltpu.VMEM((n_peers, groups, angles, rim, tile), bf16),
            pltpu.VMEM((pieces, angles, rim, tile), bf16),
            pltpu.VMEM((pieces, angles, rim, tile), bf16),
            dma((runs + 5 + angles,)),
            dma((n_others,)),
            dma((n_others,)),
            dma((2, n_peers)),
            dma((2, n_peers)),
            dma((2, 2, pieces)),
            dma((2, 2, pieces)),
        ],
        compiler_params=pltpu.CompilerParams(
            collective_id=0, has_side_effects=True, vmem_limit_bytes=VMEM
        ),
        name="project",
    )(tid, live, blocks, vol, tile_table, measured, row_norm)

    out = pl.pallas_call(
        back_kernel,
        out_shape=jax.ShapeDtypeStruct((rows, half_width), f32),
        in_specs=[hbm] * 7,
        out_specs=hbm,
        scratch_shapes=[
            chosen,
            counts,
            pltpu.VMEM((groups, angles, rim, tile), bf16),
            index,
            pltpu.VMEM(tile_table.shape, tile_table.dtype),
            pltpu.VMEM((rows, half_width), f32),
            pltpu.VMEM((rows, half_width), f32),
            pltpu.VMEM((rows, half_width), f32),
            pltpu.VMEM((angles, per_slot, tile), f32),
            pltpu.VMEM((per_slot, B_UNROLL * tile), f32),
            pltpu.SMEM((angles * slots // B_UNROLL,), jnp.int32),
            dma((6 + angles,)),
            dma((OUT_PARTS,)),
        ]
        + [pltpu.VMEM((runs * rows, tile), f32)] * ACCS,
        compiler_params=pltpu.CompilerParams(vmem_limit_bytes=VMEM),
        name="spread_back",
    )(tid, live, blocks, res, tile_table, vol, norm)
    return out.reshape(volume.shape)


def solution(mesh):
    placed = (
        P(("grp", "gz"), "gx", "row"),
        P(),
        P("gz", "gx", "row", None, None),
        P("gz", "gx", "row", None, None),
        P("gz", "gx", "row", None),
        P(("grp", "gz"), ("gx", "row"), None),
        P("gz", ("gx", "row"), None),
        P("gz", "gx", "row"),
    )
    sizes = (mesh.shape["gz"], mesh.shape["gx"], mesh.shape["row"])
    return jax.shard_map(
        functools.partial(on_device, sizes),
        mesh=mesh,
        in_specs=placed,
        out_specs=P(("grp", "gz"), "gx", "row"),
        check_vma=False,
    )
```

```python
import functools

import jax
import jax.numpy as jnp
from jax import lax
from jax.experimental import pallas as pl
from jax.experimental.pallas import tpu as pltpu
from jax.sharding import PartitionSpec as P

MESH = pl.DeviceIdType.MESH
F_UNROLL = 8
B_UNROLL = 4
ACCS = 8
OUT_PARTS = 4
VMEM = 67043328


def project_kernel(
    sizes,
    tid_hbm,
    live_hbm,
    blocks,
    vol,
    table,
    meas_hbm,
    norm_hbm,
    res,
    tid,
    live,
    meas,
    norm,
    blk,
    tbl,
    vox,
    xs,
    acc,
    padw,
    sendw,
    recvw,
    tgt,
    part,
    peer,
    rim_lo,
    rim_hi,
    local_sem,
    wsend,
    wrecv,
    psend,
    precv,
    rsend,
    rrecv,
):
    nz, nx, nr = sizes
    pieces = nx * nr
    gz, gx, row = lax.axis_index("gz"), lax.axis_index("gx"), lax.axis_index("row")
    me = gx * nr + row
    angles, slots = tid.shape
    per_slot = blocks.shape[1] // slots
    tile = table.shape[1]
    rows, width = vol.shape
    runs = width // tile
    own_angles, det_rows, cols = meas.shape
    window = sendw.shape[3]
    depth = window - 2
    block_cols = per_slot // window
    groups, _, rim, _ = res.shape

    by_run = vox.reshape(rows, runs, 1, tile)
    small = [
        pltpu.make_async_copy(meas_hbm, meas, local_sem.at[runs + 1]),
        pltpu.make_async_copy(norm_hbm, norm, local_sem.at[runs + 2]),
    ]
    copies = [
        pltpu.make_async_copy(
            vol.at[:, pl.ds(h * tile, tile)], by_run.at[:, h, 0], local_sem.at[h]
        )
        for h in range(runs)
    ]
    copies.append(pltpu.make_async_copy(table, tbl, local_sem.at[runs]))
    copies += index_copies(blocks, blk, local_sem, runs + 5)
    copies.append(pltpu.make_async_copy(tid_hbm, tid, local_sem.at[runs + 3]))
    copies.append(pltpu.make_async_copy(live_hbm, live, local_sem.at[runs + 4]))
    for copy in small + copies:
        copy.start()

    barrier = pltpu.get_barrier_semaphore()
    others = [
        (dz, dx, dr)
        for dz in range(nz)
        for dx in range(nx)
        for dr in range(nr)
        if (dz, dx, dr) != (0, 0, 0)
    ]

    def at(dz, dx, dr):
        return {
            "gz": lax.rem(gz + dz, nz),
            "gx": lax.rem(gx + dx, nx),
            "row": lax.rem(row + dr, nr),
        }

    rim_lo[...] = jnp.zeros_like(rim_lo)
    rim_hi[...] = jnp.zeros_like(rim_hi)
    for offset in others:
        pl.semaphore_signal(barrier, inc=1, device_id=at(*offset), device_id_type=MESH)

    acc[...] = jnp.zeros_like(acc)
    padw[...] = jnp.zeros_like(padw)
    for copy in small:
        copy.wait()
    for oa in range(own_angles):
        for j, ref in enumerate((meas, norm)):
            padw[j, 1 : det_rows + 1, :] = ref[oa]
        for s in range(nz):
            for j in range(2):
                sendw[s, oa, j] = padw[j, s * depth : s * depth + window, :]
    recvw[gz, me] = sendw[gz]

    for copy in copies:
        copy.wait()

    per_angle = slots // F_UNROLL
    steps = angles * per_angle

    def gather(step):
        first = step * (F_UNROLL * per_slot)
        for j in range(F_UNROLL):
            for r in range(per_slot):
                at_row = blk[first + (j * per_slot + r)]
                xs[r : r + 1, j * tile : (j + 1) * tile] = vox[at_row]

    def forward(step, carry):
        a, k0 = step // per_angle, (step % per_angle) * F_UNROLL
        x = xs[...].astype(jnp.bfloat16)
        t = live_tiles(tbl, tid, live, a, k0, F_UNROLL)
        d = lax.dot_general(x, t, (((1,), (1,)), ((), ())), preferred_element_type=jnp.float32)
        gather(jnp.minimum(step + 1, steps - 1))
        acc[a] += d
        return carry

    slab = [(dx, dr) for dx in range(nx) for dr in range(nr)]
    early = max(3 * angles // 4, 1)
    spans = [(0, early)] + ([(early, angles - early)] if early < angles else [])

    def peer_copy(phase, n):
        span = pl.ds(*spans[phase])
        return pltpu.make_async_remote_copy(
            src_ref=part.at[:, span],
            dst_ref=peer.at[n - 1, :, span],
            send_sem=psend.at[phase, n - 1],
            recv_sem=precv.at[phase, n - 1],
            device_id=at(0, *slab[n]),
            device_id_type=MESH,
        )

    def rim_copy(phase, up, n):
        span = pl.ds(*spans[phase])
        there = at(0, *slab[n])
        there["gz"] = jnp.minimum(gz + 1, nz - 1) if up else jnp.maximum(gz - 1, 0)
        return pltpu.make_async_remote_copy(
            src_ref=part.at[groups - 1 if up else 0, span],
            dst_ref=(rim_lo if up else rim_hi).at[n, span],
            send_sem=rsend.at[phase, int(up), n],
            recv_sem=rrecv.at[phase, int(up), n],
            device_id=there,
            device_id_type=MESH,
        )

    def send(phase):
        first, count = spans[phase]
        for g in range(groups):
            for a in range(first, first + count):
                part[g, a] = acc[a, g * rim : (g + 1) * rim, :].astype(part.dtype)
        for n in range(1, pieces):
            peer_copy(phase, n).start()

        @pl.when(gz < nz - 1)
        def _():
            for n in range(pieces):
                rim_copy(phase, True, n).start()

        @pl.when(gz > 0)
        def _():
            for n in range(pieces):
                rim_copy(phase, False, n).start()

    gather(jnp.int32(0))
    lax.fori_loop(0, early * per_angle, forward, 0)
    pl.semaphore_wait(barrier, len(others))
    windows = []
    for n, offset in enumerate(others):
        there = at(*offset)
        windows.append(
            pltpu.make_async_remote_copy(
                src_ref=sendw.at[there["gz"]],
                dst_ref=recvw.at[gz, me],
                send_sem=wsend.at[n],
                recv_sem=wrecv.at[n],
                device_id=there,
                device_id_type=MESH,
            )
        )
        windows[-1].start()
    send(0)
    if len(spans) > 1:
        lax.fori_loop(early * per_angle, steps, forward, 0)
        send(1)

    for copy in windows:
        copy.wait()
    per_block = tile // cols
    for z in range(nz):
        for oa in range(own_angles):
            for j in range(2):
                for b in range(block_cols):
                    cut = [recvw[z, b * per_block + i, oa, j] for i in range(per_block)]
                    value = cut[0] if per_block == 1 else jnp.concatenate(cut, axis=1)
                    tgt[j, z * own_angles + oa, pl.ds(b, window, stride=block_cols), :] = value

    for phase in range(len(spans)):
        for n in range(1, pieces):
            peer_copy(phase, n).wait()

    @pl.when(gz < nz - 1)
    def _():
        for phase in range(len(spans)):
            for n in range(pieces):
                rim_copy(phase, True, n).wait_send()
                rim_copy(phase, False, n).wait_recv()

    @pl.when(gz > 0)
    def _():
        for phase in range(len(spans)):
            for n in range(pieces):
                rim_copy(phase, False, n).wait_send()
                rim_copy(phase, True, n).wait_recv()

    for g in range(groups):
        for a in range(angles):
            total = acc[a, g * rim : (g + 1) * rim, :]
            for n in range(pieces - 1):
                total = total + peer[n, g, a].astype(jnp.float32)
            if g == 0:
                for n in range(pieces):
                    total = total + rim_lo[n, a].astype(jnp.float32)
            if g == groups - 1:
                for n in range(pieces):
                    total = total + rim_hi[n, a].astype(jnp.float32)
            rows_in = slice(g * rim, (g + 1) * rim)
            value = tgt[1, a, rows_in, :] * (tgt[0, a, rows_in, :] - total)
            res[g, a] = value.astype(res.dtype)


def index_copies(blocks, blk, sem, base):
    angles, length = blocks.shape
    return [
        pltpu.make_async_copy(blocks.at[a], blk.at[pl.ds(a * length, length)], sem.at[base + a])
        for a in range(angles)
    ]


def live_tiles(tbl, tid, live, a, k0, count):
    tiles = []
    for j in range(count):
        picked = tbl[tid[a, k0 + j]]
        tiles.append(jnp.where(k0 + j < live[a], picked, jnp.zeros_like(picked)))
    return jnp.concatenate(tiles, axis=1)


def back_kernel(
    tid_hbm, live_hbm, blocks, res_hbm, table, vol, norm, out, tid, live, res, blk, tbl, volv,
    normv, outv, rs, ss, todo, sem, out_sem, *accs
):
    angles, slots = tid.shape
    per_slot = blocks.shape[1] // slots
    tile = tbl.shape[1]
    rows, width = vol.shape
    runs = width // tile
    groups, _, rim, _ = res.shape
    small = [
        pltpu.make_async_copy(live_hbm, live, sem.at[3]),
        pltpu.make_async_copy(res_hbm, res, sem.at[4]),
    ]
    indices = [pltpu.make_async_copy(table, tbl, sem.at[2])]
    indices.append(pltpu.make_async_copy(tid_hbm, tid, sem.at[5]))
    indices += index_copies(blocks, blk, sem, 6)
    copies = [
        pltpu.make_async_copy(vol, volv, sem.at[0]),
        pltpu.make_async_copy(norm, normv, sem.at[1]),
    ]
    for copy in small + indices:
        copy.start()
    chunk = 64

    def clear(i, carry):
        for ref in accs:
            ref[pl.ds(pl.multiple_of(i * chunk, chunk), chunk), :] = jnp.zeros(
                (chunk, tile), jnp.float32
            )
        return carry

    lax.fori_loop(0, runs * rows // chunk, clear, 0)
    for copy in small:
        copy.wait()
    per_angle = slots // B_UNROLL
    count = jnp.int32(0)
    for a in range(angles):
        need = (live[a] + B_UNROLL - 1) // B_UNROLL

        def put(i, c, a=a):
            todo[c] = a * per_angle + i
            return c + 1

        count = lax.fori_loop(0, need, put, count)
        rs[a] = jnp.concatenate([res[g, a].astype(jnp.float32) for g in range(groups)], axis=0)

    for copy in indices:
        copy.wait()
    for copy in copies:
        copy.start()

    def spread(step):
        a, k0 = step // per_angle, (step % per_angle) * B_UNROLL
        t = live_tiles(tbl, tid, live, a, k0, B_UNROLL)
        return jnp.dot(rs[a].astype(jnp.bfloat16), t, preferred_element_type=jnp.float32)

    def back(i, carry):
        later = spread(todo[jnp.maximum(jnp.minimum(i + 1, count - 1), 0)])
        first = todo[i] * (B_UNROLL * per_slot)
        for j in range(B_UNROLL):
            for r in range(per_slot):
                at_row = blk[first + (j * per_slot + r)]
                accs[r % ACCS][pl.ds(at_row, 1), :] += ss[r : r + 1, j * tile : (j + 1) * tile]
        ss[...] = later
        return carry

    ss[...] = spread(todo[0])
    lax.fori_loop(0, count, back, 0)

    for copy in copies:
        copy.wait()
    size = rows // OUT_PARTS
    sub = 32
    outs = []
    for p in range(OUT_PARTS):

        def join(i, carry, p=p):
            first = pl.multiple_of(p * size + i * sub, sub)
            for h in range(runs):
                lanes = slice(h * tile, (h + 1) * tile)
                part = pl.ds(pl.multiple_of(first * runs, sub * runs), sub * runs)
                lane = pl.ds(h, sub, stride=runs)
                total = accs[0].at[part][lane, :]
                for ref in accs[1:]:
                    total = total + ref.at[part][lane, :]
                outv[pl.ds(first, sub), lanes] = (
                    volv[pl.ds(first, sub), lanes] + normv[pl.ds(first, sub), lanes] * total
                )
            return carry

        lax.fori_loop(0, size // sub, join, 0)
        part = pl.ds(p * size, size)
        outs.append(pltpu.make_async_copy(outv.at[part], out.at[part], out_sem.at[p]))
        outs[-1].start()
    for copy in outs:
        copy.wait()


def on_device(sizes, volume, tile_table, tile_ids, block_ids, live_slots, measured, row_norm, col_norm):
    nz, nx, nr = sizes
    pieces = nx * nr
    depth, column_width, half_width = volume.shape
    tile = tile_table.shape[1]
    angles, slots = tile_ids.shape[3], tile_ids.shape[4]
    window = depth + 2
    per_slot = block_ids.shape[4] // slots
    block_cols = per_slot // window
    rim = 2 * block_cols
    groups = window // 2
    runs = half_width // tile
    rows = depth * column_width
    measured = measured.transpose(0, 2, 1)
    row_norm = row_norm.transpose(0, 2, 1)
    own_angles, det_rows, cols = measured.shape
    vmem = pl.BlockSpec(memory_space=pltpu.VMEM)
    hbm = pl.BlockSpec(memory_space=pltpu.HBM)

    live = live_slots.reshape(angles)
    blocks = block_ids.reshape(angles, slots * per_slot)
    tid = tile_ids.reshape(angles, slots)
    index = pltpu.SMEM((angles * slots * per_slot,), jnp.int32)
    chosen = pltpu.SMEM((angles, slots), jnp.int32)
    counts = pltpu.SMEM((angles,), jnp.int32)
    vol = volume.reshape(rows, half_width)
    norm = col_norm.reshape(rows, half_width)
    n_others = nz * pieces - 1
    n_peers = max(pieces - 1, 1)
    dma = pltpu.SemaphoreType.DMA
    f32, bf16 = jnp.float32, jnp.bfloat16

    res = pl.pallas_call(
        functools.partial(project_kernel, sizes),
        out_shape=jax.ShapeDtypeStruct((groups, angles, rim, tile), bf16),
        in_specs=[hbm] * 7,
        out_specs=vmem,
        scratch_shapes=[
            chosen,
            counts,
            pltpu.VMEM(measured.shape, f32),
            pltpu.VMEM(measured.shape, f32),
            index,
            pltpu.VMEM(tile_table.shape, tile_table.dtype),
            pltpu.VMEM((rows * runs, 1, tile), f32),
            pltpu.VMEM((per_slot, F_UNROLL * tile), f32),
            pltpu.VMEM((angles, per_slot, tile), f32),
            pltpu.VMEM((2, det_rows + 2, cols), f32),
            pltpu.VMEM((nz, own_angles, 2, window, cols), f32),
            pltpu.VMEM((nz, pieces, own_angles, 2, window, cols), f32),
            pltpu.VMEM((2, angles, per_slot, tile), f32),
            pltpu.VMEM((groups, angles, rim, tile), bf16),
            pltpu.VMEM((n_peers, groups, angles, rim, tile), bf16),
            pltpu.VMEM((pieces, angles, rim, tile), bf16),
            pltpu.VMEM((pieces, angles, rim, tile), bf16),
            dma((runs + 5 + angles,)),
            dma((n_others,)),
            dma((n_others,)),
            dma((2, n_peers)),
            dma((2, n_peers)),
            dma((2, 2, pieces)),
            dma((2, 2, pieces)),
        ],
        compiler_params=pltpu.CompilerParams(
            collective_id=0, has_side_effects=True, vmem_limit_bytes=VMEM
        ),
        name="project",
    )(tid, live, blocks, vol, tile_table, measured, row_norm)

    out = pl.pallas_call(
        back_kernel,
        out_shape=jax.ShapeDtypeStruct((rows, half_width), f32),
        in_specs=[hbm] * 7,
        out_specs=hbm,
        scratch_shapes=[
            chosen,
            counts,
            pltpu.VMEM((groups, angles, rim, tile), bf16),
            index,
            pltpu.VMEM(tile_table.shape, tile_table.dtype),
            pltpu.VMEM((rows, half_width), f32),
            pltpu.VMEM((rows, half_width), f32),
            pltpu.VMEM((rows, half_width), f32),
            pltpu.VMEM((angles, per_slot, tile), f32),
            pltpu.VMEM((per_slot, B_UNROLL * tile), f32),
            pltpu.SMEM((angles * slots // B_UNROLL,), jnp.int32),
            dma((6 + angles,)),
            dma((OUT_PARTS,)),
        ]
        + [pltpu.VMEM((runs * rows, tile), f32)] * ACCS,
        compiler_params=pltpu.CompilerParams(vmem_limit_bytes=VMEM),
        name="spread_back",
    )(tid, live, blocks, res, tile_table, vol, norm)
    return out.reshape(volume.shape)


def solution(mesh):
    placed = (
        P(("grp", "gz"), "gx", "row"),
        P(),
        P("gz", "gx", "row", None, None),
        P("gz", "gx", "row", None, None),
        P("gz", "gx", "row", None),
        P(("grp", "gz"), ("gx", "row"), None),
        P("gz", ("gx", "row"), None),
        P("gz", "gx", "row"),
    )
    sizes = (mesh.shape["gz"], mesh.shape["gx"], mesh.shape["row"])
    return jax.shard_map(
        functools.partial(on_device, sizes),
        mesh=mesh,
        in_specs=placed,
        out_specs=P(("grp", "gz"), "gx", "row"),
        check_vma=False,
    )
```
